32 devices in a mesh: groups: 2 (over y), ep: 4 (over z), tp: 4 (over x, core).
Axes of the slice: x: 2, y: 2, z: 4, core: 2. Of those that a mesh axis runs over, the one named last changes fastest.
Arguments:
- context: bfloat16 [512, 4096], P(('groups', 'ep'), 'tp'), parts along dimension 0, may hold values from -6 to 6
- stream: bfloat16 [512, 4096], P(('groups', 'ep'), 'tp'), parts along dimension 0, may hold values from -14 to 14
- out_proj: bfloat16 [4096, 4096], P('tp', 'ep'), may hold values from -0.09375 to 0.09375
- norm_gain: bfloat16 [4096], P('tp'), may hold values from 0.099609375 to 1.8984375
- router: bfloat16 [4096, 4], P('tp'), may hold values from -0.0625 to 0.0625
- expert_ids: int32 [512, 2], P(('groups', 'ep')), parts along dimension 0, may hold values from 0 to 3, all different within a row; in each aligned block of 64 rows (0 to 63, 64 to 127, ...) at most 36 rows name the same one
- w_gate: bfloat16 [4096, 28672], P('tp', 'ep'), may hold values from -0.09375 to 0.09375
- w_up: bfloat16 [4096, 28672], P('tp', 'ep'), may hold values from -0.09375 to 0.09375
- w_down: bfloat16 [28672, 4096], P('ep', 'tp'), may hold values from -0.125 to 0.125
Outputs:
- layer_out: bfloat16 [512, 4096], P(('groups', 'ep'), 'tp'), parts along dimension 0
The draws below stay inside these ranges and needn't reach their ends.
There are 2 independent parts, one for each index of `groups`. The reference program is written for one: setup_inputs(seed, part) draws one part's arguments, and reference() takes and returns one part's arrays. A program takes and returns all parts, laid end to end along the dimension named above; an argument that names none is the same for every part. Nothing has to cross between parts.
Inputs may be any that keep to these rules, and one draw needn't show every extreme that they name: `expert_ids`: each row names 2 different experts. In each aligned block of 64 rows (the rows of one index of ep) no expert is named by more than 36 rows, and in some blocks one expert is named by exactly 36 rows.
All inputs are finite; a program needn't handle non-finite values.
Results may differ from the reference program's by a relative error of at most 0.02.
Values may be sent and summed in bfloat16 or wider, within the bound.
A program may use at most 128 MiB of HBM per device.

```python
import math
import jax
import jax.numpy as jnp
import numpy as np
from jax import lax

D = 4096
EXPERTS = 4
TOP = 2
FF = 7168
TOK = 64
ATT = 4096
CAP = 36
TOKENS = 256
N_EP = 4
N_TP = 4


def draw_stream(key, part):
    key_base, key_rows = jax.random.split(jax.random.fold_in(key, 17))
    col_scale = jnp.exp(jnp.log(3.0) * jnp.arange(D, dtype=jnp.float32) / D) / jnp.sqrt(3.0)
    noise_base = jax.random.truncated_normal(key_base, -4.0, 4.0, (TOKENS, D), jnp.float32)
    row_scale = jnp.exp(jax.random.uniform(key_rows, (TOKENS, 1), jnp.float32, jnp.log(0.2), jnp.log(2.0)))
    return (noise_base * row_scale * col_scale[None, :]).astype(jnp.bfloat16)


def shard_levels(key, dims, cuts, low, high):
    loudness, own = 1.0, jax.random.fold_in(key, 6)
    for axis_at, blocks in cuts:
        heights = jnp.exp(jax.random.uniform(jax.random.fold_in(own, axis_at), (blocks,), jnp.float32, low / len(cuts), high / len(cuts)))
        loudness = loudness * jnp.repeat(heights, dims[axis_at] // blocks).reshape([-1 if axis == axis_at else 1 for axis in range(len(dims))])
    return loudness


def assign_block(key, own, number, rows, number_of, top, most, lean):
    sequence = jax.random.permutation(key, number_of)
    heavy_load, common = shares(number_of, rows * top, most, lean, True), shares(number_of, rows * top, most, lean, False)
    places = jnp.arange(number_of)

    def named(tallies, turn):
        used = int((tallies > 0).sum())
        fixed = max(1, used // 4)
        moved = fixed + (places - fixed + turn * (used - fixed)) % max(1, number_of - fixed)
        return jnp.zeros((number_of,), jnp.int32).at[sequence[jnp.where(places < fixed, places, moved)]].set(jnp.asarray(tallies, jnp.int32))

    tallies = jnp.where(number % 4 == 0, named(heavy_load, number // 4), named(common, number - number // 4 - 1))
    mixed = jax.random.permutation(jax.random.fold_in(own, 3), number_of)
    donor, receiver = mixed[0:number_of // 2 * 2:2], mixed[1:number_of // 2 * 2:2]
    room = jnp.minimum(tallies[donor] - 1, most - tallies[receiver]) // 2
    room = jnp.where((donor == sequence[0]) | (receiver == sequence[0]) | (tallies[receiver] == 0), 0, jnp.maximum(room, 0))
    moved = jax.random.randint(jax.random.fold_in(own, 4), (number_of // 2,), 0, 1 << 20) % (room + 1)
    tallies = tallies.at[donor].add(-moved).at[receiver].add(moved)
    members = jnp.searchsorted(jnp.cumsum(tallies), jnp.arange(rows * top), side="right").astype(jnp.int32)
    listing = members.reshape(top, rows).T
    listing = listing[jax.random.permutation(jax.random.fold_in(own, 1), rows)]
    turn = jax.random.randint(jax.random.fold_in(own, 2), (rows, 1), 0, top)
    return jnp.take_along_axis(listing, (jnp.arange(top)[None, :] + turn) % top, axis=1)


def shares(number_of, total, most, lean, full):
    loads = [(1 << 20) // math.isqrt(rank ** lean) + 1 for rank in range(1, number_of + 1)]
    largest = most if full else min(most, max(-(-total // number_of), total * loads[0] // sum(loads)))
    least = 1 if total - largest >= number_of - 1 else 0
    given, surplus = [largest] + [least] * (number_of - 1), total - largest - least * (number_of - 1)
    while surplus > 0:
        free = [i for i in range(1, number_of) if given[i] < largest] or [i for i in range(1, number_of) if given[i] < most]
        pool, remaining = sum([loads[i] for i in free]), surplus
        for i in free:
            extra = min(most - given[i], max(1, remaining * loads[i] // pool), surplus)
            given[i] = given[i] + extra
            surplus = surplus - extra
    return np.array(given)


def centred(rng, dims, deviation, limit, cuts=(), kind=jnp.bfloat16):
    level = shard_levels(rng, dims, cuts, -0.22, 0.18) if cuts else 1.0
    array = jax.random.normal(rng, dims, jnp.float32) * deviation * level
    return jnp.minimum(jnp.maximum(array, -limit), limit).astype(kind)


def setup_inputs(seed: int = 0, part: int = 0) -> dict:
    splits = jax.random.split(jax.random.key(seed), 10)
    part_keys = jax.random.split(jax.random.fold_in(splits[9], part), 10)
    context = centred(part_keys[0], (TOKENS, ATT), 1.0, 6.0, ((0, 4), (1, 4)))
    stream = draw_stream(jax.random.fold_in(jax.random.fold_in(splits[9], part), 71), part)
    out_proj = centred(splits[2], (ATT, D), ATT ** -0.5, 0.09375, ((0, 4), (1, 4)))
    norm_gain = jnp.clip(1.0 + 0.18 * jax.random.normal(splits[3], (D,), jnp.float32), 0.099609375, 1.8984375).astype(jnp.bfloat16)
    router = centred(splits[4], (D, EXPERTS), (2 * D) ** -0.5, 0.0625, ((0, 4),))
    expert_ids_keys = jax.random.split(jax.random.fold_in(part_keys[5], 1), TOKENS // TOK)
    expert_ids_turns = jax.random.permutation(jax.random.fold_in(part_keys[5], 3), TOKENS // TOK)
    expert_ids = jax.vmap(lambda own, number: assign_block(jax.random.fold_in(part_keys[5], 2), own, number, TOK, EXPERTS, TOP, CAP, 2))(expert_ids_keys, expert_ids_turns).reshape((TOKENS, TOP))
    w_gate = centred(splits[6], (D, EXPERTS * FF), D ** -0.5, 0.09375, ((0, 4), (1, 4)))
    w_up = centred(splits[7], (D, EXPERTS * FF), D ** -0.5, 0.09375, ((0, 4), (1, 4)))
    w_down = centred(splits[8], (EXPERTS * FF, D), (FF // 4) ** -0.5, 0.125, ((0, 4), (1, 4)))
    return {"context": context, "stream": stream, "out_proj": out_proj, "norm_gain": norm_gain, "router": router, "expert_ids": expert_ids, "w_gate": w_gate, "w_up": w_up, "w_down": w_down}


def rounded(tensor):
    return lax.optimization_barrier(tensor.astype(jnp.bfloat16)).astype(jnp.float32)

def reference(context, stream, out_proj, norm_gain, router, expert_ids, w_gate, w_up, w_down):
    head_cols = ATT // N_TP
    attention = jnp.zeros((TOKENS, D), jnp.float32)
    for device_lane in range(N_TP):
        low_index = device_lane * head_cols
        attention = attention + rounded(jnp.dot(context[:, low_index:low_index + head_cols], out_proj[low_index:low_index + head_cols], preferred_element_type=jnp.float32))
    hstate = (stream.astype(jnp.float32) + attention).astype(jnp.bfloat16)
    hfloat = hstate.astype(jnp.float32)
    inverse = lax.rsqrt(lax.optimization_barrier(jnp.mean(hfloat * hfloat, axis=1, keepdims=True)) + 1e-05)
    normed = hfloat * inverse * norm_gain.astype(jnp.float32)
    logits = jnp.dot(normed, router.astype(jnp.float32), precision=lax.Precision.HIGHEST)
    inputs = normed.astype(jnp.bfloat16)
    experts_range = jnp.arange(EXPERTS, dtype=jnp.int32)
    picked = expert_ids[:, :, None] == experts_range[None, None, :]
    chosen = lax.optimization_barrier(jnp.sum(jnp.where(picked, logits[:, None, :], jnp.zeros_like(logits[:, None, :])), axis=2))
    leading = jax.nn.sigmoid(chosen[:, 0] - chosen[:, 1])
    weights = jnp.stack([leading, 1.0 - leading], axis=1)
    flat_ids = expert_ids.reshape(N_EP, TOK * TOP)
    onehot = (flat_ids[:, :, None] == experts_range[None, None, :]).astype(jnp.int32)
    before = jnp.cumsum(onehot, axis=1) - onehot
    slot_index = lax.optimization_barrier(jnp.sum(before * onehot, axis=2))
    block_ids = jnp.arange(N_EP, dtype=jnp.int32)[:, None]
    target = ((flat_ids * N_EP + block_ids) * CAP + slot_index).reshape(TOKENS * TOP).astype(jnp.int32)
    owner_idx = (jnp.arange(TOKENS * TOP, dtype=jnp.int32) // TOP).astype(jnp.int32)
    slot_table = jnp.full((EXPERTS * N_EP * CAP,), TOKENS, jnp.int32).at[target].set(owner_idx)
    padded = jnp.concatenate([inputs, jnp.zeros((1, D), jnp.bfloat16)], axis=0)
    rows_all = padded[slot_table].reshape(EXPERTS, N_EP * CAP, D)
    part_rows = D // N_TP
    group_size = N_EP // EXPERTS
    block_size = FF // group_size
    outputs = []
    for expert in range(EXPERTS):
        chosen_rows = rows_all[expert]
        col_base = expert * FF
        gate_sum = jnp.zeros((N_EP * CAP, FF), jnp.float32)
        up_sum = jnp.zeros((N_EP * CAP, FF), jnp.float32)
        for device_lane in range(N_TP):
            low_index = device_lane * part_rows
            row_slice = chosen_rows[:, low_index:low_index + part_rows]
            gate_sum = gate_sum + rounded(jnp.dot(row_slice, w_gate[low_index:low_index + part_rows, col_base:col_base + FF], preferred_element_type=jnp.float32))
            up_sum = up_sum + rounded(jnp.dot(row_slice, w_up[low_index:low_index + part_rows, col_base:col_base + FF], preferred_element_type=jnp.float32))
        hidden = (jax.nn.silu(gate_sum) * up_sum).astype(jnp.bfloat16)
        expert_sum = jnp.zeros((N_EP * CAP, D), jnp.float32)
        for block_id in range(group_size):
            low_index = block_id * block_size
            expert_sum = expert_sum + rounded(jnp.dot(hidden[:, low_index:low_index + block_size], w_down[col_base + low_index:col_base + low_index + block_size], preferred_element_type=jnp.float32))
        outputs.append(expert_sum)
    expert_out = jnp.concatenate(outputs, axis=0)
    gathered = expert_out[target].reshape(TOKENS, TOP, D)
    expert_mix = lax.optimization_barrier(jnp.sum(gathered * weights[:, :, None], axis=1))
    return (hfloat + expert_mix).astype(jnp.bfloat16)
```

```python
import functools

import jax
import jax.numpy as jnp
from jax import lax
from jax.experimental import pallas as pl
from jax.experimental.pallas import tpu as pltpu
from jax.sharding import PartitionSpec as P

D = 4096
EXPERTS = 4
CAP = 36


def plain_device(context, stream, out_proj, norm_gain, router, expert_ids, w_gate, w_up, w_down):
    tok_rows = stream.shape[0]
    width_part = stream.shape[1]
    ep_count = lax.axis_size("ep")
    fanout = ep_count // EXPERTS
    columns = jnp.dot(
        lax.all_gather(context, "ep", axis=0, tiled=True),
        out_proj,
        preferred_element_type=jnp.float32,
    )
    head_part = lax.all_to_all(
        columns.astype(jnp.bfloat16), "ep", split_axis=0, concat_axis=1, tiled=True
    )
    attention = lax.psum_scatter(head_part, "tp", scatter_dimension=1, tiled=True).astype(
        jnp.float32
    )
    hstate = (stream.astype(jnp.float32) + attention).astype(jnp.bfloat16)
    hfloat = hstate.astype(jnp.float32)
    gain_vec = norm_gain.astype(jnp.float32)
    router_wide = router.astype(jnp.float32)
    squares = jnp.sum(hfloat * hfloat, axis=1)
    total_sq = lax.psum(squares, "tp")
    inverse = lax.rsqrt(total_sq / D + 1e-05)[:, None]
    normed = hfloat * inverse * gain_vec[None, :]
    logits = lax.psum(jnp.dot(normed, router_wide, precision=lax.Precision.HIGHEST), "tp")
    inputs = normed.astype(jnp.bfloat16)
    experts_range = jnp.arange(EXPERTS, dtype=jnp.int32)
    flat_ids = expert_ids.reshape(tok_rows * 2)
    onehot = (flat_ids[:, None] == experts_range[None, :]).astype(jnp.int32)
    before = jnp.cumsum(onehot, axis=0) - onehot
    slot_index = jnp.sum(before * onehot, axis=1)
    target = flat_ids * CAP + slot_index
    picked = onehot.reshape(tok_rows, 2, EXPERTS).astype(jnp.float32)
    chosen = jnp.sum(picked * logits[:, None, :], axis=2)
    leading = jax.nn.sigmoid(chosen[:, 0] - chosen[:, 1])
    weights = jnp.stack([leading, 1.0 - leading], axis=1)
    columns_all = jnp.arange(EXPERTS * CAP, dtype=jnp.int32)
    placement = (
        (target[:, None] == columns_all[None, :])
        .astype(jnp.float32)
        .reshape(tok_rows, 2, EXPERTS * CAP)
    )
    dispatch = jnp.sum(placement, axis=1)
    combine = jnp.sum(placement * weights[:, :, None], axis=1)
    sectioned = lax.dot_general(
        dispatch.astype(jnp.bfloat16),
        inputs,
        (((0,), (0,)), ((), ())),
        preferred_element_type=jnp.float32,
    ).astype(jnp.bfloat16)
    send_rows = jnp.broadcast_to(
        sectioned.reshape(EXPERTS, 1, CAP, width_part), (EXPERTS, fanout, CAP, width_part)
    ).reshape(ep_count, CAP, width_part)
    received = lax.all_to_all(send_rows, "ep", split_axis=0, concat_axis=0, tiled=True)
    slot_count = received.shape[1]
    flattened = received.reshape(ep_count * slot_count, width_part)
    gate_part = jnp.dot(flattened, w_gate, preferred_element_type=jnp.float32)
    up_part = jnp.dot(flattened, w_up, preferred_element_type=jnp.float32)
    gate_sum = lax.psum(gate_part.astype(jnp.bfloat16), "tp").astype(jnp.float32)
    up_sum = lax.psum(up_part.astype(jnp.bfloat16), "tp").astype(jnp.float32)
    hidden = (jax.nn.silu(gate_sum) * up_sum).astype(jnp.bfloat16)
    partial_value = jnp.dot(hidden, w_down, preferred_element_type=jnp.float32).astype(jnp.bfloat16)
    returned_rows = lax.all_to_all(
        partial_value.reshape(ep_count, slot_count, width_part),
        "ep",
        split_axis=0,
        concat_axis=0,
        tiled=True,
    )
    summed = jnp.sum(
        returned_rows.astype(jnp.float32).reshape(EXPERTS, fanout, CAP, width_part), axis=1
    ).reshape(EXPERTS * CAP, width_part)
    expert_mix = jnp.dot(combine, summed, precision=lax.Precision.HIGHEST)
    return (hfloat + expert_mix).astype(jnp.bfloat16)


MESH = pl.DeviceIdType.MESH
CHUNK = 256
PAD = (CAP + 7) // 8 * 8
SHIFT = PAD - CAP
PACK = 2 * CAP
BASE = PACK - PAD
HOLD = 2
LAG_SUM, LAG_PASS, LAG_DOWN = 4, 7, 9
RING = 14
PIECES = 4
VMEM_BYTES = 67043328


def packed(low, high):
    return jnp.concatenate([low[:BASE], low[BASE:] + high[: PAD - BASE], high[PAD - BASE :]], axis=0)


def fused_kernel(
    n_ep,
    n_tp,
    ctx_hbm,
    stream_hbm,
    gain_hbm,
    router_hbm,
    ids_hbm,
    proj_hbm,
    gate_hbm,
    up_hbm,
    down_hbm,
    out_ref,
    ctx_all,
    stream,
    gain,
    router,
    ids,
    proj,
    gate,
    up,
    down,
    disp,
    part,
    part_in,
    halves,
    landed,
    hkeep,
    x_out,
    x_all,
    x_high,
    side,
    side_all,
    named,
    inv_out,
    inv_all,
    cols,
    pair_out,
    pair_in,
    own_far,
    own_near,
    far_out,
    far_in,
    hid,
    acc,
    outb,
    ret,
    in_sem,
    w_sem,
    ctx_send,
    ctx_recv,
    part_send,
    part_recv,
    land_send,
    land_recv,
    side_send,
    side_recv,
    x_send,
    x_recv,
    inv_send,
    inv_recv,
    ret_send,
    ret_recv,
    loop_send,
    pair_recv,
    far_recv,
    hx_recv,
    hm_recv,
):
    me = lax.axis_index("ep")
    lane = lax.axis_index("tp")
    core = lax.rem(lane, 2)
    side_x = lane // 2
    mate = 2 * side_x + (1 - core)
    across = 2 * (1 - side_x) + core
    tok, width = stream.shape
    depth = n_tp * width
    quarter = gate.shape[1] // n_tp
    count = quarter // CHUNK
    units = n_ep * count
    half = width // 2
    f32, bf16 = jnp.float32, jnp.bfloat16
    peers = (me, me + 1 - 2 * lax.rem(me, 2), lax.rem(me + 2, 4), 3 - me)
    slot_of = (0, 3, 1, 2)
    peer_of = (0, 2, 3, 1)
    middle = lax.rem((me + 1) // 2, 2)
    far_k, next_k = 3 - middle, 2 + middle
    far_peer, next_peer = 3 * (1 - me // 2), 2 - me // 2

    barrier = pltpu.get_barrier_semaphore()
    for de in range(n_ep):
        for dt in range(n_tp):
            if de or dt:
                pl.semaphore_signal(
                    barrier,
                    inc=1,
                    device_id={"ep": lax.rem(me + de, n_ep), "tp": lax.rem(lane + dt, n_tp)},
                    device_id_type=MESH,
                )

    smalls = []
    for number, (src, dst) in enumerate(
        ((ctx_hbm, ctx_all.at[0]), (ids_hbm, ids), (stream_hbm, stream), (gain_hbm, gain), (router_hbm, router))
    ):
        copy = pltpu.make_async_copy(src, dst, in_sem.at[number])
        copy.start()
        smalls.append(copy)
    weights = []
    for number, (src, dst) in enumerate(((proj_hbm, proj), (gate_hbm, gate), (up_hbm, up), (down_hbm, down))):
        step_rows = src.shape[0] // PIECES
        for p in range(PIECES):
            rows = pl.ds(p * step_rows, step_rows)
            pltpu.make_async_copy(src.at[rows], dst.at[rows], w_sem.at[number]).start()
        weights.append(pltpu.make_async_copy(src, dst, w_sem.at[number]))

    smalls[1].wait()
    kinds = lax.broadcasted_iota(jnp.int32, (8, tok), 0)
    named[0] = jnp.where(ids[0:1, :] == kinds, 1.0, 0.0).astype(f32)
    named[1] = jnp.where(ids[1:2, :] == kinds, 1.0, 0.0).astype(f32)
    both = named[0] + named[1]
    row_i = lax.broadcasted_iota(jnp.int32, (tok, tok), 0)
    col_i = lax.broadcasted_iota(jnp.int32, (tok, tok), 1)
    earlier = jnp.where(row_i < col_i, 1.0, 0.0).astype(bf16)
    rank = jnp.dot(both.astype(bf16), earlier, preferred_element_type=f32)
    rank = jnp.where(both > 0.5, rank, -4096.0)
    named[2] = rank
    slots = lax.broadcasted_iota(jnp.int32, (PAD, tok), 0).astype(f32)

    def row_of(table, k):
        return jnp.sum(jnp.where(kinds == peers[k], table, 0.0), axis=0, keepdims=True)

    for g in range(4):
        disp[g * PAD : (g + 1) * PAD] = jnp.where(row_of(rank, peer_of[g]) == slots, 1.0, 0.0).astype(f32)
    disp[4 * PAD : 5 * PAD] = jnp.where(row_of(rank, 0) + float(SHIFT) == slots, 1.0, 0.0).astype(f32)
    side[...] = jnp.zeros_like(side)
    acc[...] = jnp.zeros_like(acc)

    smalls[0].wait()
    pl.semaphore_wait(barrier, n_ep * n_tp - 1)

    def ep_copy(src, dst, slot, send, recv, target):
        return pltpu.make_async_remote_copy(
            src_ref=src,
            dst_ref=dst.at[slot],
            send_sem=send,
            recv_sem=recv.at[slot],
            device_id={"ep": target},
            device_id_type=MESH,
        )

    def ctx_copy(n, k, target):
        return ep_copy(ctx_all.at[0], ctx_all, k, ctx_send.at[n], ctx_recv, target)

    ctx_sends = (ctx_copy(0, far_k, far_peer), ctx_copy(1, next_k, next_peer), ctx_copy(2, 1, peers[1]))
    for copy in ctx_sends:
        copy.start()
    weights[0].wait()

    order = (0, 1 + middle, 2 + middle, 3 - 2 * middle)
    owners = (
        me,
        (1 - middle) * peers[1] + middle * peers[2],
        (1 - middle) * peers[2] + middle * peers[3],
        (1 - middle) * peers[3] + middle * peers[1],
    )

    def part_copy(n):
        return pltpu.make_async_remote_copy(
            src_ref=part.at[n, 1 - core],
            dst_ref=part_in.at[n],
            send_sem=part_send.at[n],
            recv_sem=part_recv.at[n],
            device_id={"tp": mate},
            device_id_type=MESH,
        )

    def land_copy(n):
        return pltpu.make_async_remote_copy(
            src_ref=halves.at[n],
            dst_ref=landed.at[lane],
            send_sem=land_send.at[n],
            recv_sem=land_recv.at[lane],
            device_id={"ep": owners[n], "tp": me},
            device_id_type=MESH,
        )

    at_home = me == lane

    def finish_part(n):
        part_copy(n).wait_recv()
        halves[n] = (part[n, core].astype(f32) + part_in[n].astype(f32)).astype(bf16)
        if n:
            land_copy(n).start()
        else:

            @pl.when(at_home)
            def _():
                landed[lane] = halves[n]

            @pl.when(jnp.logical_not(at_home))
            def _():
                land_copy(n).start()

    for n in range(4):
        if n:
            ctx_copy(0, order[n], far_peer).wait_recv()
        value = ctx_all[order[n]]
        for h in range(2):
            part[n, h] = jnp.dot(
                value, proj[:, h * half : (h + 1) * half], preferred_element_type=f32
            ).astype(bf16)
        part_copy(n).start()
        if n:
            finish_part(n - 1)
    finish_part(3)

    smalls[2].wait()
    smalls[3].wait()
    smalls[4].wait()
    for t in range(n_tp):

        @pl.when(jnp.logical_not(jnp.logical_and(at_home, lane == t)))
        def _():
            pltpu.make_async_remote_copy(
                src_ref=halves.at[0],
                dst_ref=landed.at[t],
                send_sem=land_send.at[0],
                recv_sem=land_recv.at[t],
                device_id={"tp": mate},
                device_id_type=MESH,
            ).wait_recv()

    attention = jnp.concatenate(
        [landed[h].astype(f32) + landed[2 + h].astype(f32) for h in range(2)], axis=1
    )
    hstate = (stream[...].astype(f32) + attention).astype(bf16)
    hkeep[...] = hstate
    scaled = hstate.astype(f32) * gain[...].astype(f32).reshape(1, width)
    rows = jnp.dot(disp[...].astype(bf16), scaled.astype(bf16), preferred_element_type=f32).astype(bf16)
    x_all[0] = rows[:PAD]
    for g in range(1, 4):
        x_out[g] = rows[g * PAD : (g + 1) * PAD]
    x_high[0] = rows[4 * PAD : 5 * PAD]

    def x_copy(n, slot, target):
        return pltpu.make_async_remote_copy(
            src_ref=x_out.at[slot],
            dst_ref=x_all.at[slot],
            send_sem=x_send.at[n],
            recv_sem=x_recv.at[slot],
            device_id={"ep": target},
            device_id_type=MESH,
        )

    x_sends = (x_copy(0, far_k - 1, far_peer), x_copy(1, next_k - 1, next_peer), x_copy(2, 3, peers[1]))
    for copy in x_sends:
        copy.start()

    own_q = 2 * core + side_x
    far_q = 2 * core + (1 - side_x)

    def place_of(i):
        p = lax.rem(i + HOLD, units)
        return p // count, lax.rem(p, count)

    def tp_copy(src, dst, target, number, recv):
        return pltpu.make_async_remote_copy(
            src_ref=src,
            dst_ref=dst,
            send_sem=loop_send.at[number],
            recv_sem=recv,
            device_id={"tp": target},
            device_id_type=MESH,
        )

    def pair_copy(i):
        return tp_copy(pair_out.at[i], pair_in.at[i], mate, 0, pair_recv.at[lax.rem(i, RING)])

    def far_copy(i):
        return tp_copy(far_out.at[i], far_in.at[i], across, 1, far_recv.at[lax.rem(i, RING)])

    def hid_across(i, q):
        return tp_copy(hid.at[q, i], hid.at[q, i], across, 2, hx_recv.at[lax.rem(i, RING)])

    def hid_mate(i, q, number):
        return tp_copy(hid.at[q, i], hid.at[q, i], mate, number, hm_recv.at[lax.rem(i, RING)])

    def columns_of(weight, q, chunk):
        return weight[:, pl.ds(pl.multiple_of(q * quarter + chunk * CHUNK, CHUNK), CHUNK)]

    def multiply(i):
        group, chunk = place_of(i)
        low, high = x_all[group], x_high[group]

        def block(q):
            return packed(
                jnp.dot(low, columns_of(gate, q, chunk), preferred_element_type=f32),
                jnp.dot(high, columns_of(up, q, chunk), preferred_element_type=f32),
            )

        for j in range(2):
            pair_out[i, j] = block(2 * (1 - core) + j).astype(bf16)
        own_far[lax.rem(i, 2)] = block(far_q)
        own_near[i] = block(own_q)

    def pass_far(i):
        far_out[i] = (own_far[lax.rem(i, 2)] + pair_in[i, 1 - side_x].astype(f32)).astype(bf16)

    def activate(i):
        group, _ = place_of(i)
        total = own_near[i] + pair_in[i, side_x].astype(f32) + far_in[i].astype(f32)
        scale = inv_all[group][:, 0:1]
        g = total[:PAD] * scale
        u = pltpu.roll(total[BASE:], CAP, 0) * scale
        hid[own_q, i] = (g / (1.0 + jnp.exp(-g)) * u).astype(bf16)

    def descend(i):
        group, chunk = place_of(i)
        value = acc[group]
        for q in range(4):
            value = value + jnp.dot(
                hid[q, i],
                down[pl.ds(pl.multiple_of(q * quarter + chunk * CHUNK, CHUNK), CHUNK), :],
                preferred_element_type=f32,
            )
        acc[group] = value

    def wait_mate(i):
        two = hid.at[pl.ds(2 * (1 - core), 2), i]
        tp_copy(two, two, mate, 3, hm_recv.at[lax.rem(i, RING)]).wait_recv()

    weights[1].wait()
    weights[2].wait()
    multiply(0)
    pair_copy(0).start()

    hfloat = hkeep[...].astype(f32)
    contract = (((1,), (1,)), ((), ()))
    side[0:EXPERTS, 0:tok] = lax.dot_general(
        router[...].astype(f32),
        hfloat * gain[...].astype(f32).reshape(1, width),
        contract,
        precision=lax.Precision.HIGHEST,
        preferred_element_type=f32,
    )
    side[EXPERTS:8, 0:tok] = lax.dot_general(
        jnp.ones((8, width), f32),
        hfloat * hfloat,
        contract,
        precision=lax.Precision.HIGHEST,
        preferred_element_type=f32,
    )[EXPERTS:8]

    def side_copy(k):
        return pltpu.make_async_remote_copy(
            src_ref=side,
            dst_ref=side_all.at[k - 1],
            send_sem=side_send.at[k - 1],
            recv_sem=side_recv.at[k - 1],
            device_id={"tp": lax.rem(lane + k, n_tp)},
            device_id_type=MESH,
        )

    for k in range(1, n_tp):
        side_copy(k).start()

    def inv_copy(k):
        return ep_copy(inv_out.at[slot_of[k]], inv_all, slot_of[k], inv_send.at[k - 1], inv_recv, peers[k])

    def finish_side():
        total = side[...]
        for k in range(1, n_tp):
            side_copy(k).wait_recv()
            total = total + side_all[k - 1]
        total = total[:, 0:tok]
        inverse = lax.rsqrt(total[EXPERTS : EXPERTS + 1] / depth + 1e-05)
        logits = total * inverse
        first = jnp.sum(named[0] * logits, axis=0, keepdims=True)
        second = jnp.sum(named[1] * logits, axis=0, keepdims=True)
        leading = jax.nn.sigmoid(first - second)
        mix = named[0] * leading + named[1] * (1.0 - leading)
        inverse_cols = jnp.transpose(jnp.broadcast_to(inverse, (128, tok)))
        spread = jnp.dot(
            disp[0 : 4 * PAD],
            inverse_cols,
            precision=lax.Precision.HIGHEST,
            preferred_element_type=f32,
        )
        for g in range(4):
            inv_out[g] = spread[g * PAD : (g + 1) * PAD]
        inv_all[0] = spread[:PAD]
        for k in range(1, n_ep):
            inv_copy(k).start()
        places = [row_of(named[2], k) for k in range(4)] + [row_of(mix, k) for k in range(4)]
        cols[...] = jnp.transpose(
            jnp.concatenate(places + [jnp.zeros((120, tok), f32)], axis=0)
        )

    shifted = jnp.where(
        lax.broadcasted_iota(jnp.int32, (PAD, PAD), 0)
        == lax.broadcasted_iota(jnp.int32, (PAD, PAD), 1) + SHIFT,
        1.0,
        0.0,
    ).astype(bf16)

    def take_rows(g):
        x_copy(0, g, me).wait_recv()
        x_high[g] = jnp.dot(shifted, x_all[g], preferred_element_type=f32).astype(bf16)

    def ret_copy(g):
        k = peer_of[g]
        return ep_copy(outb.at[g], ret, k, ret_send.at[g - 1], ret_recv, peers[k])

    lane_i = lax.broadcasted_iota(jnp.int32, (tok, PAD), 1).astype(f32)

    def returned(k, value):
        chosen = jnp.where(cols[:, k : k + 1] == lane_i, 1.0, 0.0).astype(bf16)
        return cols[:, 4 + k : 5 + k] * jnp.dot(chosen, value, preferred_element_type=f32)

    def within(i, when, act):
        if when is None:
            return
        if when:
            act()
        else:
            pl.when(jnp.logical_and(i >= 0, i < units))(act)

    def step(s, multiplying, others):
        i_down, i_pass, i_sum, i_far = s - LAG_DOWN, s - LAG_PASS, s - LAG_SUM, s - 1

        for g in range(1, 4):

            @pl.when(s == g * count - HOLD)
            def _():
                take_rows(g)

            @pl.when(s == g * count - HOLD + LAG_SUM)
            def _():
                inv_copy(peer_of[g]).wait_recv()

        @pl.when(s == LAG_SUM)
        def _():
            finish_side()

        def do_far():
            pair_copy(i_far).wait_recv()
            pass_far(i_far)
            far_copy(i_far).start()

        def do_sum():
            far_copy(i_sum).wait_recv()
            activate(i_sum)
            hid_across(i_sum, own_q).start()
            hid_mate(i_sum, own_q, 3).start()

        def do_pass():
            hid_across(i_pass, far_q).wait_recv()
            hid_mate(i_pass, far_q, 4).start()

        def do_down():
            wait_mate(i_down)
            descend(i_down)

        def do_both():
            wait_mate(i_down)
            multiply(s)
            descend(i_down)
            pair_copy(s).start()

        within(i_far, others, do_far)
        within(i_sum, others, do_sum)
        within(i_pass, others, do_pass)
        if multiplying and others:
            do_both()
        else:
            if multiplying:
                multiply(s)
                pair_copy(s).start()
            within(i_down, others, do_down)

        for g in range(1, 4):

            @pl.when(i_down == (g + 1) * count - 1 - HOLD)
            def _():
                outb[g] = acc[g].astype(bf16)
                ret_copy(g).start()

    def early(s, carry):
        step(s, True, False)
        return carry

    def steady(s, carry):
        step(s, True, True)
        return carry

    def late(s, carry):
        step(s, False, False)
        return carry

    lax.fori_loop(1, LAG_DOWN, early, 0)
    weights[3].wait()
    lax.fori_loop(LAG_DOWN, units, steady, 0)
    lax.fori_loop(units, units + LAG_DOWN, late, 0)

    result = hkeep[...].astype(f32) + returned(0, acc[0].astype(bf16))
    for k in (2, 3, 1):
        ep_copy(outb.at[1], ret, k, ret_send.at[0], ret_recv, me).wait_recv()
        result = result + returned(k, ret[k])
    out_ref[...] = result.astype(bf16)

    for copy in ctx_sends + x_sends:
        copy.wait_send()
    for n in range(4):
        part_copy(n).wait_send()
        if n:
            land_copy(n).wait_send()

    @pl.when(jnp.logical_not(at_home))
    def _():
        land_copy(0).wait_send()

    for k in range(1, 4):
        side_copy(k).wait_send()
        inv_copy(k).wait_send()
        ret_copy(k).wait_send()
    tp_copy(pair_out, pair_in, mate, 0, pair_recv.at[0]).wait_send()
    tp_copy(far_out, far_in, across, 1, far_recv.at[0]).wait_send()
    for q, target, number in ((own_q, across, 2), (own_q, mate, 3), (far_q, mate, 4)):
        tp_copy(hid.at[q], hid.at[q], target, number, hx_recv.at[0]).wait_send()


def fused_device(context, stream, out_proj, norm_gain, router, expert_ids, w_gate, w_up, w_down):
    n_ep, n_tp = lax.axis_size("ep"), lax.axis_size("tp")
    tok, width = stream.shape
    heads = context.shape[1]
    units = n_ep * (w_gate.shape[1] // n_tp // CHUNK)
    bf16, f32 = jnp.bfloat16, jnp.float32
    hbm = pl.BlockSpec(memory_space=pl.ANY)
    vmem = pl.BlockSpec(memory_space=pltpu.VMEM)
    arrays = [
        ((n_ep, tok, heads), bf16),
        (stream.shape, bf16),
        (norm_gain.shape, bf16),
        (router.shape[::-1], bf16),
        (expert_ids.shape[::-1], jnp.int32),
        (out_proj.shape, bf16),
        (w_gate.shape, bf16),
        (w_up.shape, bf16),
        (w_down.shape, bf16),
        ((5 * PAD, tok), f32),
        ((n_ep, 2, tok, width // 2), bf16),
        ((n_ep, tok, width // 2), bf16),
        ((n_ep, tok, width // 2), bf16),
        ((n_tp, tok, width // 2), bf16),
        ((tok, width), bf16),
        ((n_ep, PAD, width), bf16),
        ((n_ep, PAD, width), bf16),
        ((n_ep, PAD, width), bf16),
        ((8, 128), f32),
        ((n_tp - 1, 8, 128), f32),
        ((3, 8, tok), f32),
        ((n_ep, PAD, 128), f32),
        ((n_ep, PAD, 128), f32),
        ((tok, 128), f32),
        ((units, 2, PACK, CHUNK), bf16),
        ((units, 2, PACK, CHUNK), bf16),
        ((2, PACK, CHUNK), f32),
        ((units, PACK, CHUNK), f32),
        ((units, PACK, CHUNK), bf16),
        ((units, PACK, CHUNK), bf16),
        ((n_tp, units, PAD, CHUNK), bf16),
        ((n_ep, PAD, width), f32),
        ((n_ep, PAD, width), bf16),
        ((n_ep, PAD, width), bf16),
    ]
    scratch = [pltpu.VMEM(shape, kind) for shape, kind in arrays]
    for size in (5, 4, 3, 4, 4, 4, 4, 4, 3, 3, 3, 4, 3, 4, 3, 4, 5, RING, RING, RING, RING):
        scratch.append(pltpu.SemaphoreType.DMA((size,)))
    return pl.pallas_call(
        functools.partial(fused_kernel, n_ep, n_tp),
        out_shape=jax.ShapeDtypeStruct((tok, width), bf16),
        in_specs=[hbm] * 9,
        out_specs=vmem,
        scratch_shapes=scratch,
        compiler_params=pltpu.CompilerParams(
            collective_id=0, has_side_effects=True, vmem_limit_bytes=VMEM_BYTES
        ),
        name="fused_layer",
    )(context, stream, norm_gain, router.T, expert_ids.T, out_proj, w_gate, w_up, w_down)


def solution(mesh):
    sizes = dict(mesh.shape)
    fused = sizes["tp"] == 4 and sizes["ep"] == EXPERTS
    return jax.shard_map(
        fused_device if fused else plain_device,
        mesh=mesh,
        in_specs=(
            P(("groups", "ep"), "tp"),
            P(("groups", "ep"), "tp"),
            P("tp", "ep"),
            P("tp"),
            P("tp", None),
            P(("groups", "ep"), None),
            P("tp", "ep"),
            P("tp", "ep"),
            P("ep", "tp"),
        ),
        out_specs=P(("groups", "ep"), "tp"),
        check_vma=False,
    )
```

```python
import functools

import jax
import jax.numpy as jnp
from jax import lax
from jax.experimental import pallas as pl
from jax.experimental.pallas import tpu as pltpu
from jax.sharding import PartitionSpec as P

D = 4096
EXPERTS = 4
CAP = 36


def plain_device(context, stream, out_proj, norm_gain, router, expert_ids, w_gate, w_up, w_down):
    tok_rows = stream.shape[0]
    width_part = stream.shape[1]
    ep_count = lax.axis_size("ep")
    fanout = ep_count // EXPERTS
    columns = jnp.dot(
        lax.all_gather(context, "ep", axis=0, tiled=True),
        out_proj,
        preferred_element_type=jnp.float32,
    )
    head_part = lax.all_to_all(
        columns.astype(jnp.bfloat16), "ep", split_axis=0, concat_axis=1, tiled=True
    )
    attention = lax.psum_scatter(head_part, "tp", scatter_dimension=1, tiled=True).astype(
        jnp.float32
    )
    hstate = (stream.astype(jnp.float32) + attention).astype(jnp.bfloat16)
    hfloat = hstate.astype(jnp.float32)
    gain_vec = norm_gain.astype(jnp.float32)
    router_wide = router.astype(jnp.float32)
    squares = jnp.sum(hfloat * hfloat, axis=1)
    total_sq = lax.psum(squares, "tp")
    inverse = lax.rsqrt(total_sq / D + 1e-05)[:, None]
    normed = hfloat * inverse * gain_vec[None, :]
    logits = lax.psum(jnp.dot(normed, router_wide, precision=lax.Precision.HIGHEST), "tp")
    inputs = normed.astype(jnp.bfloat16)
    experts_range = jnp.arange(EXPERTS, dtype=jnp.int32)
    flat_ids = expert_ids.reshape(tok_rows * 2)
    onehot = (flat_ids[:, None] == experts_range[None, :]).astype(jnp.int32)
    before = jnp.cumsum(onehot, axis=0) - onehot
    slot_index = jnp.sum(before * onehot, axis=1)
    target = flat_ids * CAP + slot_index
    picked = onehot.reshape(tok_rows, 2, EXPERTS).astype(jnp.float32)
    chosen = jnp.sum(picked * logits[:, None, :], axis=2)
    leading = jax.nn.sigmoid(chosen[:, 0] - chosen[:, 1])
    weights = jnp.stack([leading, 1.0 - leading], axis=1)
    columns_all = jnp.arange(EXPERTS * CAP, dtype=jnp.int32)
    placement = (
        (target[:, None] == columns_all[None, :])
        .astype(jnp.float32)
        .reshape(tok_rows, 2, EXPERTS * CAP)
    )
    dispatch = jnp.sum(placement, axis=1)
    combine = jnp.sum(placement * weights[:, :, None], axis=1)
    sectioned = lax.dot_general(
        dispatch.astype(jnp.bfloat16),
        inputs,
        (((0,), (0,)), ((), ())),
        preferred_element_type=jnp.float32,
    ).astype(jnp.bfloat16)
    send_rows = jnp.broadcast_to(
        sectioned.reshape(EXPERTS, 1, CAP, width_part), (EXPERTS, fanout, CAP, width_part)
    ).reshape(ep_count, CAP, width_part)
    received = lax.all_to_all(send_rows, "ep", split_axis=0, concat_axis=0, tiled=True)
    slot_count = received.shape[1]
    flattened = received.reshape(ep_count * slot_count, width_part)
    gate_part = jnp.dot(flattened, w_gate, preferred_element_type=jnp.float32)
    up_part = jnp.dot(flattened, w_up, preferred_element_type=jnp.float32)
    gate_sum = lax.psum(gate_part.astype(jnp.bfloat16), "tp").astype(jnp.float32)
    up_sum = lax.psum(up_part.astype(jnp.bfloat16), "tp").astype(jnp.float32)
    hidden = (jax.nn.silu(gate_sum) * up_sum).astype(jnp.bfloat16)
    partial_value = jnp.dot(hidden, w_down, preferred_element_type=jnp.float32).astype(jnp.bfloat16)
    returned_rows = lax.all_to_all(
        partial_value.reshape(ep_count, slot_count, width_part),
        "ep",
        split_axis=0,
        concat_axis=0,
        tiled=True,
    )
    summed = jnp.sum(
        returned_rows.astype(jnp.float32).reshape(EXPERTS, fanout, CAP, width_part), axis=1
    ).reshape(EXPERTS * CAP, width_part)
    expert_mix = jnp.dot(combine, summed, precision=lax.Precision.HIGHEST)
    return (hfloat + expert_mix).astype(jnp.bfloat16)


MESH = pl.DeviceIdType.MESH
CHUNK = 256
PAD = (CAP + 7) // 8 * 8
SHIFT = PAD - CAP
PACK = 2 * CAP
BASE = PACK - PAD
HOLD = 2
LAG_SUM, LAG_PASS, LAG_DOWN = 4, 8, 10
SEND_AT = 1
RING = 14
PIECES = 4
VMEM_BYTES = 67043328


def packed(low, high):
    return jnp.concatenate([low[:BASE], low[BASE:] + high[: PAD - BASE], high[PAD - BASE :]], axis=0)


def fused_kernel(
    n_ep,
    n_tp,
    ctx_hbm,
    stream_hbm,
    gain_hbm,
    router_hbm,
    ids_hbm,
    proj_hbm,
    gate_hbm,
    up_hbm,
    down_hbm,
    out_ref,
    ctx_all,
    stream,
    gain,
    router,
    ids,
    proj,
    gate,
    up,
    down,
    disp,
    part,
    part_in,
    halves,
    landed,
    hkeep,
    x_out,
    x_all,
    x_high,
    side,
    side_all,
    named,
    inv_out,
    inv_all,
    cols,
    pair_out,
    pair_in,
    own_far,
    own_near,
    far_out,
    far_in,
    hid,
    acc,
    outb,
    ret,
    in_sem,
    w_sem,
    ctx_send,
    ctx_recv,
    part_send,
    part_recv,
    land_send,
    land_recv,
    side_send,
    side_recv,
    x_send,
    x_recv,
    inv_send,
    inv_recv,
    ret_send,
    ret_recv,
    loop_send,
    pair_recv,
    far_recv,
    hx_recv,
    hm_recv,
):
    me = lax.axis_index("ep")
    lane = lax.axis_index("tp")
    core = lax.rem(lane, 2)
    side_x = lane // 2
    mate = 2 * side_x + (1 - core)
    across = 2 * (1 - side_x) + core
    tok, width = stream.shape
    depth = n_tp * width
    quarter = gate.shape[1] // n_tp
    count = quarter // CHUNK
    units = n_ep * count
    half = width // 2
    f32, bf16 = jnp.float32, jnp.bfloat16
    peers = (me, me + 1 - 2 * lax.rem(me, 2), lax.rem(me + 2, 4), 3 - me)
    slot_of = (0, 3, 1, 2)
    peer_of = (0, 2, 3, 1)
    middle = lax.rem((me + 1) // 2, 2)
    far_k, next_k = 3 - middle, 2 + middle
    far_peer, next_peer = 3 * (1 - me // 2), 2 - me // 2

    barrier = pltpu.get_barrier_semaphore()
    for de in range(n_ep):
        for dt in range(n_tp):
            if de or dt:
                pl.semaphore_signal(
                    barrier,
                    inc=1,
                    device_id={"ep": lax.rem(me + de, n_ep), "tp": lax.rem(lane + dt, n_tp)},
                    device_id_type=MESH,
                )

    smalls = []
    for number, (src, dst) in enumerate(
        ((ctx_hbm, ctx_all.at[0]), (ids_hbm, ids), (stream_hbm, stream), (gain_hbm, gain), (router_hbm, router))
    ):
        copy = pltpu.make_async_copy(src, dst, in_sem.at[number])
        copy.start()
        smalls.append(copy)
    weights = []
    for number, (src, dst) in enumerate(((proj_hbm, proj), (gate_hbm, gate), (up_hbm, up), (down_hbm, down))):
        weights.append((src, dst, pltpu.make_async_copy(src, dst, w_sem.at[number])))

    def load(number):
        src, dst, _ = weights[number]
        step_rows = src.shape[0] // PIECES
        for p in range(PIECES):
            rows = pl.ds(p * step_rows, step_rows)
            pltpu.make_async_copy(src.at[rows], dst.at[rows], w_sem.at[number]).start()

    load(0)

    smalls[1].wait()
    kinds = lax.broadcasted_iota(jnp.int32, (8, tok), 0)
    named[0] = jnp.where(ids[0:1, :] == kinds, 1.0, 0.0).astype(f32)
    named[1] = jnp.where(ids[1:2, :] == kinds, 1.0, 0.0).astype(f32)
    both = named[0] + named[1]
    row_i = lax.broadcasted_iota(jnp.int32, (tok, tok), 0)
    col_i = lax.broadcasted_iota(jnp.int32, (tok, tok), 1)
    earlier = jnp.where(row_i < col_i, 1.0, 0.0).astype(bf16)
    rank = jnp.dot(both.astype(bf16), earlier, preferred_element_type=f32)
    rank = jnp.where(both > 0.5, rank, -4096.0)
    named[2] = rank
    slots = lax.broadcasted_iota(jnp.int32, (PAD, tok), 0).astype(f32)

    def row_of(table, k):
        return jnp.sum(jnp.where(kinds == peers[k], table, 0.0), axis=0, keepdims=True)

    for g in range(4):
        disp[g * PAD : (g + 1) * PAD] = jnp.where(row_of(rank, peer_of[g]) == slots, 1.0, 0.0).astype(f32)
    disp[4 * PAD : 5 * PAD] = jnp.where(row_of(rank, 0) + float(SHIFT) == slots, 1.0, 0.0).astype(f32)
    side[...] = jnp.zeros_like(side)
    acc[...] = jnp.zeros_like(acc)

    for n in (0, 2, 3, 4):
        smalls[n].wait()
    for n in (1, 2, 3):
        load(n)
    pl.semaphore_wait(barrier, n_ep * n_tp - 1)

    def ep_copy(src, dst, slot, send, recv, target):
        return pltpu.make_async_remote_copy(
            src_ref=src,
            dst_ref=dst.at[slot],
            send_sem=send,
            recv_sem=recv.at[slot],
            device_id={"ep": target},
            device_id_type=MESH,
        )

    def ctx_copy(n, k, target):
        return ep_copy(ctx_all.at[0], ctx_all, k, ctx_send.at[n], ctx_recv, target)

    ctx_sends = (ctx_copy(0, far_k, far_peer), ctx_copy(1, next_k, next_peer), ctx_copy(2, 1, peers[1]))
    for copy in ctx_sends:
        copy.start()
    weights[0][2].wait()

    order = (0, 1 + middle, 2 + middle, 3 - 2 * middle)
    owners = (
        me,
        (1 - middle) * peers[1] + middle * peers[2],
        (1 - middle) * peers[2] + middle * peers[3],
        (1 - middle) * peers[3] + middle * peers[1],
    )

    def part_copy(n):
        return pltpu.make_async_remote_copy(
            src_ref=part.at[n, 1 - core],
            dst_ref=part_in.at[n],
            send_sem=part_send.at[n],
            recv_sem=part_recv.at[n],
            device_id={"tp": mate},
            device_id_type=MESH,
        )

    def land_copy(n):
        return pltpu.make_async_remote_copy(
            src_ref=halves.at[n],
            dst_ref=landed.at[lane],
            send_sem=land_send.at[n],
            recv_sem=land_recv.at[lane],
            device_id={"ep": owners[n], "tp": me},
            device_id_type=MESH,
        )

    at_home = me == lane

    def finish_part(n):
        part_copy(n).wait_recv()
        halves[n] = (part[n, core].astype(f32) + part_in[n].astype(f32)).astype(bf16)
        if n:
            land_copy(n).start()
        else:

            @pl.when(at_home)
            def _():
                landed[lane] = halves[n]

            @pl.when(jnp.logical_not(at_home))
            def _():
                land_copy(n).start()

    for n in range(4):
        if n:
            ctx_copy(0, order[n], far_peer).wait_recv()
        value = ctx_all[order[n]]
        for h in range(2):
            part[n, h] = jnp.dot(
                value, proj[:, h * half : (h + 1) * half], preferred_element_type=f32
            ).astype(bf16)
        part_copy(n).start()
        if n:
            finish_part(n - 1)
    finish_part(3)

    for t in range(n_tp):

        @pl.when(jnp.logical_not(jnp.logical_and(at_home, lane == t)))
        def _():
            pltpu.make_async_remote_copy(
                src_ref=halves.at[0],
                dst_ref=landed.at[t],
                send_sem=land_send.at[0],
                recv_sem=land_recv.at[t],
                device_id={"tp": mate},
                device_id_type=MESH,
            ).wait_recv()

    attention = jnp.concatenate(
        [landed[h].astype(f32) + landed[2 + h].astype(f32) for h in range(2)], axis=1
    )
    hstate = (stream[...].astype(f32) + attention).astype(bf16)
    hkeep[...] = hstate
    scaled = hstate.astype(f32) * gain[...].astype(f32).reshape(1, width)
    rows = jnp.dot(disp[...].astype(bf16), scaled.astype(bf16), preferred_element_type=f32).astype(bf16)
    x_all[0] = rows[:PAD]
    for g in range(1, 4):
        x_out[g] = rows[g * PAD : (g + 1) * PAD]
    x_high[0] = rows[4 * PAD : 5 * PAD]

    def x_copy(n, slot, target):
        return pltpu.make_async_remote_copy(
            src_ref=x_out.at[slot],
            dst_ref=x_all.at[slot],
            send_sem=x_send.at[n],
            recv_sem=x_recv.at[slot],
            device_id={"ep": target},
            device_id_type=MESH,
        )

    x_sends = (x_copy(0, far_k - 1, far_peer), x_copy(1, next_k - 1, next_peer), x_copy(2, 3, peers[1]))

    own_q = 2 * core + side_x
    far_q = 2 * core + (1 - side_x)

    def place_of(i):
        p = lax.rem(i + HOLD, units)
        return p // count, lax.rem(p, count)

    def tp_copy(src, dst, target, number, recv):
        return pltpu.make_async_remote_copy(
            src_ref=src,
            dst_ref=dst,
            send_sem=loop_send.at[number],
            recv_sem=recv,
            device_id={"tp": target},
            device_id_type=MESH,
        )

    def pair_copy(i):
        return tp_copy(pair_out.at[i], pair_in.at[i], mate, 0, pair_recv.at[lax.rem(i, RING)])

    def far_copy(i):
        return tp_copy(far_out.at[i], far_in.at[i], across, 1, far_recv.at[lax.rem(i, RING)])

    def hid_across(i, q):
        return tp_copy(hid.at[q, i], hid.at[q, i], across, 2, hx_recv.at[lax.rem(i, RING)])

    def hid_mate(i, q, number):
        return tp_copy(hid.at[q, i], hid.at[q, i], mate, number, hm_recv.at[lax.rem(i, RING)])

    def columns_of(weight, q, chunk):
        return weight[:, pl.ds(pl.multiple_of(q * quarter + chunk * CHUNK, CHUNK), CHUNK)]

    def multiply(i):
        group, chunk = place_of(i)
        low, high = x_all[group], x_high[group]

        def block(q):
            return packed(
                jnp.dot(low, columns_of(gate, q, chunk), preferred_element_type=f32),
                jnp.dot(high, columns_of(up, q, chunk), preferred_element_type=f32),
            )

        for j in range(2):
            pair_out[i, j] = block(2 * (1 - core) + j).astype(bf16)
        own_far[lax.rem(i, 2)] = block(far_q)
        own_near[i] = block(own_q)

    def pass_far(i):
        far_out[i] = (own_far[lax.rem(i, 2)] + pair_in[i, 1 - side_x].astype(f32)).astype(bf16)

    def activate(i):
        group, _ = place_of(i)
        total = own_near[i] + pair_in[i, side_x].astype(f32) + far_in[i].astype(f32)
        scale = inv_all[group][:, 0:1]
        g = total[:PAD] * scale
        u = pltpu.roll(total[BASE:], CAP, 0) * scale
        hid[own_q, i] = (g / (1.0 + jnp.exp(-g)) * u).astype(bf16)

    def descend(i):
        group, chunk = place_of(i)
        value = acc[group]
        for q in range(4):
            value = value + jnp.dot(
                hid[q, i],
                down[pl.ds(pl.multiple_of(q * quarter + chunk * CHUNK, CHUNK), CHUNK), :],
                preferred_element_type=f32,
            )
        acc[group] = value

    def wait_mate(i):
        two = hid.at[pl.ds(2 * (1 - core), 2), i]
        tp_copy(two, two, mate, 3, hm_recv.at[lax.rem(i, RING)]).wait_recv()

    weights[1][2].wait()
    weights[2][2].wait()
    multiply(0)
    pair_copy(0).start()

    hfloat = hkeep[...].astype(f32)
    contract = (((1,), (1,)), ((), ()))
    side[0:EXPERTS, 0:tok] = lax.dot_general(
        router[...].astype(f32),
        hfloat * gain[...].astype(f32).reshape(1, width),
        contract,
        precision=lax.Precision.HIGHEST,
        preferred_element_type=f32,
    )
    side[EXPERTS:8, 0:tok] = lax.dot_general(
        jnp.ones((8, width), f32),
        hfloat * hfloat,
        contract,
        precision=lax.Precision.HIGHEST,
        preferred_element_type=f32,
    )[EXPERTS:8]

    def side_copy(k):
        return pltpu.make_async_remote_copy(
            src_ref=side,
            dst_ref=side_all.at[k - 1],
            send_sem=side_send.at[k - 1],
            recv_sem=side_recv.at[k - 1],
            device_id={"tp": lax.rem(lane + k, n_tp)},
            device_id_type=MESH,
        )

    for k in range(1, n_tp):
        side_copy(k).start()

    def inv_copy(k):
        return ep_copy(inv_out.at[slot_of[k]], inv_all, slot_of[k], inv_send.at[k - 1], inv_recv, peers[k])

    def finish_side():
        total = side[...]
        for k in range(1, n_tp):
            side_copy(k).wait_recv()
            total = total + side_all[k - 1]
        total = total[:, 0:tok]
        inverse = lax.rsqrt(total[EXPERTS : EXPERTS + 1] / depth + 1e-05)
        logits = total * inverse
        first = jnp.sum(named[0] * logits, axis=0, keepdims=True)
        second = jnp.sum(named[1] * logits, axis=0, keepdims=True)
        leading = jax.nn.sigmoid(first - second)
        mix = named[0] * leading + named[1] * (1.0 - leading)
        inverse_cols = jnp.transpose(jnp.broadcast_to(inverse, (128, tok)))
        spread = jnp.dot(
            disp[0 : 4 * PAD],
            inverse_cols,
            precision=lax.Precision.HIGHEST,
            preferred_element_type=f32,
        )
        for g in range(4):
            inv_out[g] = spread[g * PAD : (g + 1) * PAD]
        inv_all[0] = spread[:PAD]
        for k in range(1, n_ep):
            inv_copy(k).start()
        places = [row_of(named[2], k) for k in range(4)] + [row_of(mix, k) for k in range(4)]
        cols[...] = jnp.transpose(
            jnp.concatenate(places + [jnp.zeros((120, tok), f32)], axis=0)
        )

    shifted = jnp.where(
        lax.broadcasted_iota(jnp.int32, (PAD, PAD), 0)
        == lax.broadcasted_iota(jnp.int32, (PAD, PAD), 1) + SHIFT,
        1.0,
        0.0,
    ).astype(bf16)

    def take_rows(g):
        x_copy(0, g, me).wait_recv()
        x_high[g] = jnp.dot(shifted, x_all[g], preferred_element_type=f32).astype(bf16)

    def ret_copy(g):
        k = peer_of[g]
        return ep_copy(outb.at[g], ret, k, ret_send.at[g - 1], ret_recv, peers[k])

    lane_i = lax.broadcasted_iota(jnp.int32, (tok, PAD), 1).astype(f32)

    def returned(k, value):
        chosen = jnp.where(cols[:, k : k + 1] == lane_i, 1.0, 0.0).astype(bf16)
        return cols[:, 4 + k : 5 + k] * jnp.dot(chosen, value, preferred_element_type=f32)

    def within(i, when, act):
        if when is None:
            return
        if when:
            act()
        else:
            pl.when(jnp.logical_and(i >= 0, i < units))(act)

    def send_rows():
        for copy in x_sends:
            copy.start()

    def step(s, multiplying, others):
        i_down, i_pass, i_sum, i_far = s - LAG_DOWN, s - LAG_PASS, s - LAG_SUM, s - 1

        for g in range(1, 4):

            @pl.when(s == g * count - HOLD)
            def _():
                take_rows(g)

            @pl.when(s == g * count - HOLD + LAG_SUM)
            def _():
                inv_copy(peer_of[g]).wait_recv()

        @pl.when(s == SEND_AT)
        def _():
            send_rows()

        @pl.when(s == LAG_SUM)
        def _():
            finish_side()

        def do_far():
            pair_copy(i_far).wait_recv()
            pass_far(i_far)
            far_copy(i_far).start()

        def do_sum():
            far_copy(i_sum).wait_recv()
            activate(i_sum)
            hid_across(i_sum, own_q).start()
            hid_mate(i_sum, own_q, 3).start()

        def do_pass():
            hid_across(i_pass, far_q).wait_recv()
            hid_mate(i_pass, far_q, 4).start()

        def do_down():
            wait_mate(i_down)
            descend(i_down)

        def do_both():
            wait_mate(i_down)
            multiply(s)
            descend(i_down)
            pair_copy(s).start()

        if multiplying and others:
            do_both()
        elif multiplying:
            multiply(s)
            pair_copy(s).start()
        within(i_far, others, do_far)
        within(i_sum, others, do_sum)
        within(i_pass, others, do_pass)
        if not (multiplying and others):
            within(i_down, others, do_down)

        for g in range(1, 4):

            @pl.when(i_down == (g + 1) * count - 1 - HOLD)
            def _():
                outb[g] = acc[g].astype(bf16)
                ret_copy(g).start()

    def early(s, carry):
        step(s, True, False)
        return carry

    def steady(s, carry):
        step(s, True, True)
        return carry

    def late(s, carry):
        step(s, False, False)
        return carry

    lax.fori_loop(1, LAG_DOWN, early, 0)
    weights[3][2].wait()
    lax.fori_loop(LAG_DOWN, units, steady, 0)
    lax.fori_loop(units, units + LAG_DOWN, late, 0)

    result = hkeep[...].astype(f32) + returned(0, acc[0].astype(bf16))
    for k in (2, 3, 1):
        ep_copy(outb.at[1], ret, k, ret_send.at[0], ret_recv, me).wait_recv()
        result = result + returned(k, ret[k])
    out_ref[...] = result.astype(bf16)

    for copy in ctx_sends + x_sends:
        copy.wait_send()
    for n in range(4):
        part_copy(n).wait_send()
        if n:
            land_copy(n).wait_send()

    @pl.when(jnp.logical_not(at_home))
    def _():
        land_copy(0).wait_send()

    for k in range(1, 4):
        side_copy(k).wait_send()
        inv_copy(k).wait_send()
        ret_copy(k).wait_send()
    tp_copy(pair_out, pair_in, mate, 0, pair_recv.at[0]).wait_send()
    tp_copy(far_out, far_in, across, 1, far_recv.at[0]).wait_send()
    for q, target, number in ((own_q, across, 2), (own_q, mate, 3), (far_q, mate, 4)):
        tp_copy(hid.at[q], hid.at[q], target, number, hx_recv.at[0]).wait_send()


def fused_device(context, stream, out_proj, norm_gain, router, expert_ids, w_gate, w_up, w_down):
    n_ep, n_tp = lax.axis_size("ep"), lax.axis_size("tp")
    tok, width = stream.shape
    heads = context.shape[1]
    units = n_ep * (w_gate.shape[1] // n_tp // CHUNK)
    bf16, f32 = jnp.bfloat16, jnp.float32
    hbm = pl.BlockSpec(memory_space=pl.ANY)
    vmem = pl.BlockSpec(memory_space=pltpu.VMEM)
    arrays = [
        ((n_ep, tok, heads), bf16),
        (stream.shape, bf16),
        (norm_gain.shape, bf16),
        (router.shape[::-1], bf16),
        (expert_ids.shape[::-1], jnp.int32),
        (out_proj.shape, bf16),
        (w_gate.shape, bf16),
        (w_up.shape, bf16),
        (w_down.shape, bf16),
        ((5 * PAD, tok), f32),
        ((n_ep, 2, tok, width // 2), bf16),
        ((n_ep, tok, width // 2), bf16),
        ((n_ep, tok, width // 2), bf16),
        ((n_tp, tok, width // 2), bf16),
        ((tok, width), bf16),
        ((n_ep, PAD, width), bf16),
        ((n_ep, PAD, width), bf16),
        ((n_ep, PAD, width), bf16),
        ((8, 128), f32),
        ((n_tp - 1, 8, 128), f32),
        ((3, 8, tok), f32),
        ((n_ep, PAD, 128), f32),
        ((n_ep, PAD, 128), f32),
        ((tok, 128), f32),
        ((units, 2, PACK, CHUNK), bf16),
        ((units, 2, PACK, CHUNK), bf16),
        ((2, PACK, CHUNK), f32),
        ((units, PACK, CHUNK), f32),
        ((units, PACK, CHUNK), bf16),
        ((units, PACK, CHUNK), bf16),
        ((n_tp, units, PAD, CHUNK), bf16),
        ((n_ep, PAD, width), f32),
        ((n_ep, PAD, width), bf16),
        ((n_ep, PAD, width), bf16),
    ]
    scratch = [pltpu.VMEM(shape, kind) for shape, kind in arrays]
    for size in (5, 4, 3, 4, 4, 4, 4, 4, 3, 3, 3, 4, 3, 4, 3, 4, 5, RING, RING, RING, RING):
        scratch.append(pltpu.SemaphoreType.DMA((size,)))
    return pl.pallas_call(
        functools.partial(fused_kernel, n_ep, n_tp),
        out_shape=jax.ShapeDtypeStruct((tok, width), bf16),
        in_specs=[hbm] * 9,
        out_specs=vmem,
        scratch_shapes=scratch,
        compiler_params=pltpu.CompilerParams(
            collective_id=0, has_side_effects=True, vmem_limit_bytes=VMEM_BYTES
        ),
        name="fused_layer",
    )(context, stream, norm_gain, router.T, expert_ids.T, out_proj, w_gate, w_up, w_down)


def solution(mesh):
    sizes = dict(mesh.shape)
    fused = sizes["tp"] == 4 and sizes["ep"] == EXPERTS
    return jax.shard_map(
        fused_device if fused else plain_device,
        mesh=mesh,
        in_specs=(
            P(("groups", "ep"), "tp"),
            P(("groups", "ep"), "tp"),
            P("tp", "ep"),
            P("tp"),
            P("tp", None),
            P(("groups", "ep"), None),
            P("tp", "ep"),
            P("tp", "ep"),
            P("ep", "tp"),
        ),
        out_specs=P(("groups", "ep"), "tp"),
        check_vma=False,
    )
```
